32 devices in a mesh: rep: 2 (over x), dp: 16 (over y, z, core).
Axes of the slice: x: 2, y: 2, z: 4, core: 2. Of those that a mesh axis runs over, the one named last changes fastest.
Arguments:
- x: bfloat16 [32, 2048, 1024], P(('rep', 'dp')), parts along dimension 0
- dy: bfloat16 [32, 2048, 1024], P(('rep', 'dp')), parts along dimension 0
- w_gate: bfloat16 [2, 1024, 4096], replicated
- w_up: bfloat16 [2, 1024, 4096], replicated
- w_down: bfloat16 [2, 4096, 1024], replicated
- m_w_gate: float32 [2, 1024, 4096], P(None, 'dp')
- m_w_up: float32 [2, 1024, 4096], P(None, 'dp')
- m_w_down: float32 [2, 4096, 1024], P(None, 'dp')
- v_w_gate: float32 [2, 1024, 4096], P(None, 'dp')
- v_w_up: float32 [2, 1024, 4096], P(None, 'dp')
- v_w_down: float32 [2, 4096, 1024], P(None, 'dp')
Outputs:
- output 1: bfloat16 [4, 1024, 4096], P('rep'), parts along dimension 0
- output 2: bfloat16 [4, 1024, 4096], P('rep'), parts along dimension 0
- output 3: bfloat16 [4, 4096, 1024], P('rep'), parts along dimension 0
- output 4: float32 [4, 1024, 4096], P('rep', 'dp'), parts along dimension 0
- output 5: float32 [4, 1024, 4096], P('rep', 'dp'), parts along dimension 0
- output 6: float32 [4, 4096, 1024], P('rep', 'dp'), parts along dimension 0
- output 7: float32 [4, 1024, 4096], P('rep', 'dp'), parts along dimension 0
- output 8: float32 [4, 1024, 4096], P('rep', 'dp'), parts along dimension 0
- output 9: float32 [4, 4096, 1024], P('rep', 'dp'), parts along dimension 0
There are 2 independent parts. The reference program is written for one: setup_inputs(seed, part) draws one part's arguments, and reference() takes and returns one part's arrays. A program takes and returns all parts, laid end to end along the dimension named above; an argument that names none is the same for every part.
All inputs are finite; a program needn't handle non-finite values.
Results may differ from the reference program's by a relative error of at most 0.022.
Values are sent between devices in bfloat16 or wider.
A program may use at most 2 GiB of HBM per device.

```python
import jax
import jax.numpy as jnp
from jax import lax

SEQUENCES = 16
TOKENS = 2048
D = 1024
FF = 4096
LAYERS = 2
NAMES = ("w_gate", "w_up", "w_down")
SHAPES = {"w_gate": (LAYERS, D, FF), "w_up": (LAYERS, D, FF), "w_down": (LAYERS, FF, D)}


def bump(key, n, height):
    away = (jnp.arange(n, dtype=jnp.int32) - jax.random.randint(key, (), 0, n, jnp.int32)) % n
    return jnp.where(away < n // 8, height, 1.0)


def together(key, own, strength):
    shared = jax.random.normal(key, own.shape[1:], jnp.float32)
    return (own + strength * shared) * lax.rsqrt(1 + strength * strength)


def setup_inputs(seed: int = 0, part: int = 0) -> dict:
    kx, kdy, ka, kb, kz, kf, kh, kl, *keys = jax.random.split(jax.random.key(seed), 8 + 3 * len(NAMES))
    kx, kdy, ka, kb = (jax.random.fold_in(k, part) for k in (kx, kdy, ka, kb))
    kw, km, kv = (keys[i::3] for i in range(3))
    shape = (SEQUENCES, TOKENS, D)
    much_x, much_dy = jax.random.uniform(kz, (2,), jnp.float32, 0.0, 1.0)
    loud = 2.0 ** jax.random.uniform(jax.random.fold_in(kz, 1), (), jnp.float32, -1.0, 2.0)
    layers = 2.0 ** jax.random.uniform(kl, (LAYERS, 1, 1), jnp.float32, -1.0, 1.0)
    x = together(ka, jax.random.normal(kx, shape, jnp.float32), much_x) * bump(kf, D, 4.0)
    dy = together(kb, jax.random.normal(kdy, shape, jnp.float32), much_dy)
    drawn = {"x": x.astype(jnp.bfloat16), "dy": (loud * dy * (SEQUENCES * TOKENS) ** -0.5).astype(jnp.bfloat16)}
    for key, name in zip(kw, NAMES, strict=True):
        w = jax.random.normal(key, SHAPES[name], jnp.float32) * SHAPES[name][1] ** -0.5
        drawn[name] = (w * {"w_gate": 1.0, "w_up": bump(kh, FF, 4.0), "w_down": layers}[name]).astype(jnp.bfloat16)
    for key, name in zip(km, NAMES, strict=True):
        drawn[f"m_{name}"] = 0.1 * jax.random.normal(key, SHAPES[name], jnp.float32)
    for key, name in zip(kv, NAMES, strict=True):
        drawn[f"v_{name}"] = jax.random.uniform(key, SHAPES[name], jnp.float32, 0.005, 0.015)
    return drawn


def matmul(a, w):
    return jnp.dot(a, w, preferred_element_type=jnp.float32).astype(jnp.bfloat16)


def normed(h):
    wide = h.astype(jnp.float32)
    scale = lax.rsqrt(jnp.mean(wide**2, -1, keepdims=True) + 1e-6)
    return (wide * scale).astype(jnp.bfloat16)


def layer(h, w):
    a = normed(h)
    gate = jnp.dot(a, w["w_gate"], preferred_element_type=jnp.float32)
    up = jnp.dot(a, w["w_up"], preferred_element_type=jnp.float32)
    return h + matmul((jax.nn.silu(gate) * up).astype(jnp.bfloat16), w["w_down"])


def adamw(w, m, v, g):
    m = 0.9 * m + 0.1 * g
    v = 0.95 * v + 0.05 * g * g
    step = m * lax.rsqrt(v + 1e-8) + 0.1 * w
    return (w - 0.02 * step).astype(jnp.bfloat16), m, v


def clipped(gradients, sum_of_squares, count):
    factor = jnp.minimum(1.0, 0.5 * lax.rsqrt(sum_of_squares / count + 1e-30))
    return [g * factor for g in gradients]


def stack(weights, h):
    return lax.scan(lambda h, w: (layer(h, w), None), h, weights)[0]


def reference(x, dy, w_gate, w_up, w_down, m_w_gate, m_w_up, m_w_down, v_w_gate, v_w_up, v_w_down):
    weights = dict(zip(NAMES, (w_gate, w_up, w_down), strict=True))

    def take(so_far, sequence):
        h, by_y = sequence
        _, back = jax.vjp(lambda w: stack(w, h), weights)
        return jax.tree.map(lambda total, term: total + term.astype(jnp.float32), so_far, back(by_y)[0]), None

    none_yet = {name: jnp.zeros(w.shape, jnp.float32) for name, w in weights.items()}
    by_weights, _ = lax.scan(take, none_yet, (x, dy))
    gradients = [by_weights[name].astype(jnp.bfloat16).astype(jnp.float32) for name in NAMES]
    gradients = clipped(gradients, sum(jnp.sum(g * g) for g in gradients), sum(g.size for g in gradients))
    new = [
        adamw(w.astype(jnp.float32), m, v, g)
        for w, m, v, g in zip((w_gate, w_up, w_down), (m_w_gate, m_w_up, m_w_down), (v_w_gate, v_w_up, v_w_down), gradients, strict=True)
    ]
    return tuple(one[which] for which in range(3) for one in new)
```

```python
import jax
import jax.numpy as jnp
from jax import lax
from jax.sharding import PartitionSpec as P

NAMES = ("w_gate", "w_up", "w_down")
F32, BF16 = jnp.float32, jnp.bfloat16


def dot(a, b, ca, cb):
    return lax.dot_general(a, b, (((ca,), (cb,)), ((), ())), preferred_element_type=F32)


def normed(h):
    wide = h.astype(F32)
    scale = lax.rsqrt(jnp.mean(wide**2, -1, keepdims=True) + 1e-6)
    return (wide * scale).astype(BF16)


def act(gate, up):
    return (jax.nn.silu(gate) * up).astype(BF16)


def act_back(gate, up, dhid):
    d = dhid.astype(F32)
    s = jax.nn.sigmoid(gate)
    silu = gate * s
    return (d * up * (s * (1 + gate * (1 - s)))).astype(BF16), (d * silu).astype(BF16)


def adamw(w, m, v, g):
    m = 0.9 * m + 0.1 * g
    v = 0.95 * v + 0.05 * g * g
    step = m * lax.rsqrt(v + 1e-8) + 0.1 * w
    return (w - 0.02 * step).astype(BF16), m, v


def solution(mesh):
    n = mesh.shape["dp"]

    def body(x, dy, wg, wu, wd, *mv):
        h0, dy = x[0], dy[0]
        m, v = mv[:3], mv[3:]

        def scatter(g):
            return lax.psum_scatter(g, "dp", scatter_dimension=0, tiled=True)

        a0 = normed(h0)
        g0, u0 = dot(a0, wg[0], 1, 0), dot(a0, wu[0], 1, 0)
        hid0 = act(g0, u0)
        h1 = h0 + dot(hid0, wd[0], 1, 0).astype(BF16)
        a1, norm_back = jax.vjp(normed, h1)
        g1, u1 = dot(a1, wg[1], 1, 0), dot(a1, wu[1], 1, 0)
        hid1 = act(g1, u1)
        d_down1 = scatter(dot(hid1, dy, 0, 0).astype(BF16))
        dhid1 = dot(dy, wd[1], 1, 1).astype(BF16)
        dg1, du1 = act_back(g1, u1, dhid1)
        d_gate1 = scatter(dot(a1, dg1, 0, 0).astype(BF16))
        d_up1 = scatter(dot(a1, du1, 0, 0).astype(BF16))
        da1 = dot(dg1, wg[1], 1, 1).astype(BF16) + dot(du1, wu[1], 1, 1).astype(BF16)
        dh1 = dy + norm_back(da1)[0]
        d_down0 = scatter(dot(hid0, dh1, 0, 0).astype(BF16))
        dhid0 = dot(dh1, wd[0], 1, 1).astype(BF16)
        dg0, du0 = act_back(g0, u0, dhid0)
        d_gate0 = scatter(dot(a0, dg0, 0, 0).astype(BF16))
        d_up0 = scatter(dot(a0, du0, 0, 0).astype(BF16))
        gs = [(d_gate0, d_gate1), (d_up0, d_up1), (d_down0, d_down1)]
        total = sum(jnp.sum(jnp.square(g.astype(F32))) for pair in gs for g in pair)
        total = lax.psum(total, "dp")
        count = sum(w.size for w in (wg, wu, wd))
        factor = jnp.minimum(1.0, 0.5 * lax.rsqrt(total / count + 1e-30))
        me = lax.axis_index("dp")
        news, ms, vs = [], [], []
        for w, mm, vv, pair in zip((wg, wu, wd), m, v, gs):
            rows = w.shape[1] // n
            own = lax.dynamic_slice_in_dim(w, me * rows, rows, 1)
            g = jnp.stack([p.astype(F32) for p in pair]) * factor
            new, nm, nv = adamw(own.astype(F32), mm, vv, g)
            news.append(lax.all_gather(new, "dp", axis=1, tiled=True))
            ms.append(nm)
            vs.append(nv)
        return (*news, *ms, *vs)

    seq, whole, shard = P(("rep", "dp")), P(), P(None, "dp")
    return jax.shard_map(
        body,
        mesh=mesh,
        in_specs=(seq, seq, whole, whole, whole, *([shard] * 6)),
        out_specs=(*([P("rep")] * 3), *([P("rep", "dp")] * 6)),
        check_vma=False,
    )
```

```python
import functools

import jax
import jax.numpy as jnp
from jax import lax
from jax.experimental import pallas as pl
from jax.experimental.pallas import tpu as pltpu
from jax.sharding import PartitionSpec as P

NAMES = ("w_gate", "w_up", "w_down")
F32, BF16 = jnp.float32, jnp.bfloat16
MESH = pl.DeviceIdType.MESH


def dot(a, b, ca, cb):
    return lax.dot_general(a, b, (((ca,), (cb,)), ((), ())), preferred_element_type=F32)


def normed(h):
    wide = h.astype(F32)
    scale = lax.rsqrt(jnp.mean(wide**2, -1, keepdims=True) + 1e-6)
    return (wide * scale).astype(BF16)


def act(gate, up):
    return (jax.nn.silu(gate) * up).astype(BF16)


def act_back(gate, up, dhid):
    d = dhid.astype(F32)
    s = jax.nn.sigmoid(gate)
    silu = gate * s
    return (d * up * (s * (1 + gate * (1 - s)))).astype(BF16), (d * silu).astype(BF16)


def adamw(w, m, v, g):
    m = 0.9 * m + 0.1 * g
    v = 0.95 * v + 0.05 * g * g
    step = m * lax.rsqrt(v + 1e-8) + 0.1 * w
    return (w - 0.02 * step).astype(BF16), m, v


def place(n):
    me = lax.axis_index("dp")
    core, chip = me % 2, me // 2
    half = n // 4
    pos = chip + (chip // half) * (3 * half - 1 - 2 * chip)

    def owner(p, c):
        return 2 * (p + (p // half) * (3 * half - 1 - 2 * p)) + c

    return core, pos, owner


def entry_barrier(devices):
    sem = pltpu.get_barrier_semaphore()
    for d in devices:
        pl.semaphore_signal(sem, inc=1, device_id={"dp": d}, device_id_type=MESH)
    pl.semaphore_wait(sem, len(devices))


def remote(src, dst, send, recv, dev):
    return pltpu.make_async_remote_copy(
        src_ref=src, dst_ref=dst, send_sem=send, recv_sem=recv, device_id={"dp": dev}, device_id_type=MESH
    )


def gather_kernel(n, rows, *refs):
    k = len(rows)
    ins, outs, bufs = refs[:k], refs[k : 2 * k], refs[2 * k : 3 * k]
    ring_send, ring_recv, d2d_send, d2d_recv, local = refs[3 * k :]
    chips = n // 2
    core, pos, owner = place(n)
    right, left = owner((pos + 1) % chips, core), owner((pos + chips - 1) % chips, core)
    partner = owner(pos, 1 - core)
    entry_barrier((left, right, partner))
    to = (right, left)

    def out_rows(i, way, s, c):
        q = (pos + (chips - s if way == 0 else s)) % chips
        h = rows[i] // 2
        return outs[i].at[:, pl.ds(pl.multiple_of(owner(q, c) * rows[i] + way * h, h), h)]

    def hop(i, way, s):
        return remote(bufs[i].at[way, s], bufs[i].at[way, s + 1], ring_send.at[i, way, s], ring_recv.at[i, way, s], to[way])

    def across(i, way, s, c):
        return remote(bufs[i].at[way, s], out_rows(i, way, s, c), d2d_send.at[i, way, s], d2d_recv.at[i, way, s], partner)

    def keep(i, way, s):
        return pltpu.make_async_copy(bufs[i].at[way, s], out_rows(i, way, s, core), local.at[i, way, s])

    def load(i, way):
        h = rows[i] // 2
        return pltpu.make_async_copy(ins[i].at[:, pl.ds(way * h, h)], bufs[i].at[way, 0], local.at[i, way, chips])

    every = [(i, way) for i in range(k) for way in range(2)]
    for i, way in every:
        load(i, way).start()
    for s in range(chips):
        for i, way in every:
            if s == 0:
                load(i, way).wait()
            else:
                hop(i, way, s - 1).wait_recv()
            if s < chips - 1:
                hop(i, way, s).start()
            across(i, way, s, core).start()
            keep(i, way, s).start()
    for s in range(chips):
        for i, way in every:
            if s < chips - 1:
                hop(i, way, s).wait_send()
            across(i, way, s, core).wait_send()
            across(i, way, s, 1 - core).wait_recv()
            keep(i, way, s).wait()


def gather(n, blocks, collective_id):
    k, chips = len(blocks), n // 2
    rows = [b.shape[1] for b in blocks]
    sems = [pltpu.SemaphoreType.DMA((k, 2, chips))] * 4 + [pltpu.SemaphoreType.DMA((k, 2, chips + 1))]
    sent = 2 * sum(b.size * 2 for b in blocks) * (chips - 1)
    return pl.pallas_call(
        functools.partial(gather_kernel, n, rows),
        out_shape=[jax.ShapeDtypeStruct((b.shape[0], n * b.shape[1], b.shape[2]), b.dtype) for b in blocks],
        in_specs=[pl.BlockSpec(memory_space=pl.ANY)] * k,
        out_specs=[pl.BlockSpec(memory_space=pl.ANY)] * k,
        scratch_shapes=[pltpu.VMEM((2, chips, b.shape[0], b.shape[1] // 2, b.shape[2]), b.dtype) for b in blocks] + sems,
        compiler_params=pltpu.CompilerParams(collective_id=collective_id, has_side_effects=True, vmem_limit_bytes=60 << 20),
        name="gather_weights",
    )(*blocks)


def solution(mesh):
    n = mesh.shape["dp"]

    def body(x, dy, wg, wu, wd, *mv):
        h0, dy = x[0], dy[0]
        m, v = mv[:3], mv[3:]

        def scatter(g):
            return lax.psum_scatter(g, "dp", scatter_dimension=0, tiled=True)

        a0 = normed(h0)
        g0, u0 = dot(a0, wg[0], 1, 0), dot(a0, wu[0], 1, 0)
        hid0 = act(g0, u0)
        h1 = h0 + dot(hid0, wd[0], 1, 0).astype(BF16)
        a1, norm_back = jax.vjp(normed, h1)
        g1, u1 = dot(a1, wg[1], 1, 0), dot(a1, wu[1], 1, 0)
        hid1 = act(g1, u1)
        d_down1 = scatter(dot(hid1, dy, 0, 0).astype(BF16))
        dhid1 = dot(dy, wd[1], 1, 1).astype(BF16)
        dg1, du1 = act_back(g1, u1, dhid1)
        d_gate1 = scatter(dot(a1, dg1, 0, 0).astype(BF16))
        d_up1 = scatter(dot(a1, du1, 0, 0).astype(BF16))
        da1 = dot(dg1, wg[1], 1, 1).astype(BF16) + dot(du1, wu[1], 1, 1).astype(BF16)
        dh1 = dy + norm_back(da1)[0]
        d_down0 = scatter(dot(hid0, dh1, 0, 0).astype(BF16))
        dhid0 = dot(dh1, wd[0], 1, 1).astype(BF16)
        dg0, du0 = act_back(g0, u0, dhid0)
        d_gate0 = scatter(dot(a0, dg0, 0, 0).astype(BF16))
        d_up0 = scatter(dot(a0, du0, 0, 0).astype(BF16))
        gs = [(d_gate0, d_gate1), (d_up0, d_up1), (d_down0, d_down1)]
        total = sum(jnp.sum(jnp.square(g.astype(F32))) for pair in gs for g in pair)
        total = lax.psum(total, "dp")
        count = sum(w.size for w in (wg, wu, wd))
        factor = jnp.minimum(1.0, 0.5 * lax.rsqrt(total / count + 1e-30))
        me = lax.axis_index("dp")
        news, ms, vs = [], [], []
        for w, mm, vv, pair in zip((wg, wu, wd), m, v, gs):
            rows = w.shape[1] // n
            own = lax.dynamic_slice_in_dim(w, me * rows, rows, 1)
            g = jnp.stack([p.astype(F32) for p in pair]) * factor
            new, nm, nv = adamw(own.astype(F32), mm, vv, g)
            news.append(new)
            ms.append(nm)
            vs.append(nv)
        return (*gather(n, news, 0), *ms, *vs)

    seq, whole, shard = P(("rep", "dp")), P(), P(None, "dp")
    return jax.shard_map(
        body,
        mesh=mesh,
        in_specs=(seq, seq, whole, whole, whole, *([shard] * 6)),
        out_specs=(*([P("rep")] * 3), *([P("rep", "dp")] * 6)),
        check_vma=False,
    )
```

```python
import functools

import jax
import jax.numpy as jnp
from jax import lax
from jax.experimental import pallas as pl
from jax.experimental.pallas import tpu as pltpu
from jax.sharding import PartitionSpec as P

F32, BF16 = jnp.float32, jnp.bfloat16
MESH = pl.DeviceIdType.MESH
TILE = 512


def dot(a, b, ca, cb):
    return lax.dot_general(a, b, (((ca,), (cb,)), ((), ())), preferred_element_type=F32)


def normed(h):
    wide = h.astype(F32)
    scale = lax.rsqrt(jnp.mean(wide**2, -1, keepdims=True) + 1e-6)
    return (wide * scale).astype(BF16)


def act(gate, up):
    return (jax.nn.silu(gate) * up).astype(BF16)


def act_back(gate, up, dhid):
    d = dhid.astype(F32)
    s = jax.nn.sigmoid(gate)
    silu = gate * s
    return (d * up * (s * (1 + gate * (1 - s)))).astype(BF16), (d * silu).astype(BF16)


def adamw(w, m, v, g):
    m = 0.9 * m + 0.1 * g
    v = 0.95 * v + 0.05 * g * g
    step = m * lax.rsqrt(v + 1e-8) + 0.1 * w
    return (w - 0.02 * step).astype(BF16), m, v


def place(n):
    me = lax.axis_index("dp")
    core, chip = me % 2, me // 2
    half = n // 4
    pos = chip + (chip // half) * (3 * half - 1 - 2 * chip)

    def owner(p, c):
        return 2 * (p + (p // half) * (3 * half - 1 - 2 * p)) + c

    return core, pos, owner


def entry_barrier(devices):
    sem = pltpu.get_barrier_semaphore()
    for d in devices:
        pl.semaphore_signal(sem, inc=1, device_id={"dp": d}, device_id_type=MESH)
    pl.semaphore_wait(sem, len(devices))


def remote(src, dst, send, recv, dev):
    return pltpu.make_async_remote_copy(
        src_ref=src, dst_ref=dst, send_sem=send, recv_sem=recv, device_id={"dp": dev}, device_id_type=MESH
    )


def gather_kernel(n, rows, *refs):
    k = len(rows)
    ins, outs, bufs = refs[:k], refs[k : 2 * k], refs[2 * k : 3 * k]
    ring_send, ring_recv, d2d_send, d2d_recv, local = refs[3 * k :]
    chips = n // 2
    core, pos, owner = place(n)
    right, left = owner((pos + 1) % chips, core), owner((pos + chips - 1) % chips, core)
    partner = owner(pos, 1 - core)
    entry_barrier((left, right, partner))
    to = (right, left)

    def out_rows(i, way, s, c):
        q = (pos + (chips - s if way == 0 else s)) % chips
        h = rows[i] // 2
        return outs[i].at[:, pl.ds(pl.multiple_of(owner(q, c) * rows[i] + way * h, h), h)]

    def hop(i, way, s):
        return remote(bufs[i].at[way, s], bufs[i].at[way, s + 1], ring_send.at[i, way, s], ring_recv.at[i, way, s], to[way])

    def across(i, way, s, c):
        return remote(bufs[i].at[way, s], out_rows(i, way, s, c), d2d_send.at[i, way, s], d2d_recv.at[i, way, s], partner)

    def keep(i, way, s):
        return pltpu.make_async_copy(bufs[i].at[way, s], out_rows(i, way, s, core), local.at[i, way, s])

    def load(i, way):
        h = rows[i] // 2
        return pltpu.make_async_copy(ins[i].at[:, pl.ds(way * h, h)], bufs[i].at[way, 0], local.at[i, way, chips])

    every = [(i, way) for i in range(k) for way in range(2)]
    for i, way in every:
        load(i, way).start()
    for s in range(chips):
        for i, way in every:
            if s == 0:
                load(i, way).wait()
            else:
                hop(i, way, s - 1).wait_recv()
            if s < chips - 1:
                hop(i, way, s).start()
            across(i, way, s, core).start()
            keep(i, way, s).start()
    for s in range(chips):
        for i, way in every:
            if s < chips - 1:
                hop(i, way, s).wait_send()
            across(i, way, s, core).wait_send()
            across(i, way, s, 1 - core).wait_recv()
            keep(i, way, s).wait()


def gather(n, blocks, collective_id):
    k, chips = len(blocks), n // 2
    rows = [b.shape[1] for b in blocks]
    sems = [pltpu.SemaphoreType.DMA((k, 2, chips))] * 4 + [pltpu.SemaphoreType.DMA((k, 2, chips + 1))]
    return pl.pallas_call(
        functools.partial(gather_kernel, n, rows),
        out_shape=[jax.ShapeDtypeStruct((b.shape[0], n * b.shape[1], b.shape[2]), b.dtype) for b in blocks],
        in_specs=[pl.BlockSpec(memory_space=pl.ANY)] * k,
        out_specs=[pl.BlockSpec(memory_space=pl.ANY)] * k,
        scratch_shapes=[pltpu.VMEM((2, chips, b.shape[0], b.shape[1] // 2, b.shape[2]), b.dtype) for b in blocks] + sems,
        compiler_params=pltpu.CompilerParams(collective_id=collective_id, has_side_effects=True, vmem_limit_bytes=60 << 20),
        name="gather_weights",
    )(*blocks)


def summed(refs, cols, step=512):
    total = refs[0][:, pl.ds(cols, step)].astype(F32)
    for r in refs[1:]:
        total += r[:, pl.ds(cols, step)].astype(F32)
    return total


def last_kernel(n, refs_in, refs_out, own, made, tiles, got, buf, sems):
    down, a_t, *by_hidden = refs_in
    own_sem, d2d_send, d2d_recv, ring_send, ring_recv, tile_sem = sems
    chips, k = n // 2, 3
    grads = (down, made.at[0], made.at[1])
    rows = [g.shape[0] // n for g in grads]
    wide = [g.shape[1] // 2 for g in grads]
    core, pos, owner = place(n)
    right, left = owner((pos + 1) % chips, core), owner((pos + chips - 1) % chips, core)
    partner = owner(pos, 1 - core)
    entry_barrier((left, right, partner))
    to = (right, left)

    def start_row(i, d, c, more=0):
        at = owner((pos + d) % chips, c) * rows[i] + more
        return pl.multiple_of(at, rows[i] // 2)

    def load(d):
        return pltpu.make_async_copy(down.at[pl.ds(start_row(0, d, core), rows[0])], own.at[d], own_sem.at[d])

    def cross(i, d):
        src = grads[i].at[pl.ds(start_row(i, d, 1 - core), rows[i])]
        return remote(src, got[i].at[d], d2d_send.at[i, d], d2d_recv.at[i, d], partner)

    def hop(i, part, way, s):
        cols = pl.ds(part * wide[i], wide[i])
        return remote(
            buf[i].at[way, s, :, cols],
            buf[i].at[way, s + 1, :, cols],
            ring_send.at[i, part, way, s],
            ring_recv.at[i, part, way, s],
            to[way],
        )

    order = list(dict.fromkeys(d % chips for s in range(chips) for d in (chips - 1 - s, 1 + s)))

    def begin(i):
        for d in order:
            cross(i, d).start()
            if i == 0:
                load(d).start()

    ready = set()

    def turn(i, number):
        part, s = number % 2, number // 2
        h = rows[i] // 2
        for way in range(2):
            d = (chips - 1 - s if way == 0 else 1 + s) % chips
            if (i, d) not in ready:
                ready.add((i, d))
                if i == 0:
                    load(d).wait()
                cross(i, d).wait_recv()
            if s > 0:
                hop(i, part, way, s - 1).wait_recv()
            half = pl.ds(way * h, h)
            mine = own.at[d, half] if i == 0 else grads[i].at[pl.ds(start_row(i, d, core, way * h), h)]
            terms = [mine, got[i].at[d, half]] + ([buf[i].at[way, s]] if s > 0 else [])
            result = buf[i].at[way, s] if s < chips - 1 else refs_out[i].at[half]

            def add(c, _, terms=terms, result=result, part=part, i=i):
                at = pl.multiple_of(part * wide[i] + c * 512, 512)
                result[:, pl.ds(at, 512)] = summed(terms, at).astype(BF16)
                return 0

            lax.fori_loop(0, wide[i] // 512, add, 0)
            if s < chips - 1:
                hop(i, part, way, s).start()

    per = by_hidden[0].shape[1] // TILE
    count = 2 * per

    def fetch(t):
        src = by_hidden[t // per].at[:, pl.ds(t % per * TILE, TILE)]
        return pltpu.make_async_copy(src, tiles.at[t % 2], tile_sem.at[t % 2])

    high = min(512, a_t.shape[0])
    begin(0)
    fetch(0).start()
    gate, up = list(range(2 * chips)), list(range(2 * chips))
    for t in range(count):
        fetch(t).wait()
        if t + 1 < count:
            fetch(t + 1).start()

        def matmul(m, _, t=t):
            at = pl.ds(pl.multiple_of(m * high, high), high)
            made[t // per, at, pl.ds(t % per * TILE, TILE)] = jnp.dot(
                a_t[at], tiles[t % 2], preferred_element_type=F32
            ).astype(BF16)
            return 0

        lax.fori_loop(0, a_t.shape[0] // high, matmul, 0)
        for number in range(t * 2 * chips // count, (t + 1) * 2 * chips // count):
            turn(0, number)
        if t == per - 1:
            begin(1)
        if t > per:
            turn(1, gate.pop(0))
    begin(2)
    while gate or up:
        if gate:
            turn(1, gate.pop(0))
        if up:
            turn(2, up.pop(0))
    for i in range(k):
        for d in range(chips):
            cross(i, d).wait_send()
        for part in range(2):
            for way in range(2):
                for s in range(chips - 1):
                    hop(i, part, way, s).wait_send()


def last_gradients(n, down, a_t, by_gate, by_up, collective_id):
    chips, k = n // 2, 3
    shapes = [down.shape, (a_t.shape[0], by_gate.shape[1]), (a_t.shape[0], by_up.shape[1])]
    rows = [s[0] // n for s in shapes]
    dma = pltpu.SemaphoreType.DMA
    scratch = (
        [pltpu.VMEM((chips, rows[0], shapes[0][1]), BF16), pltpu.VMEM((2, *shapes[1]), BF16), pltpu.VMEM((2, a_t.shape[1], TILE), BF16)]
        + [pltpu.VMEM((chips, r, s[1]), BF16) for r, s in zip(rows, shapes)]
        + [pltpu.VMEM((2, chips, r // 2, s[1]), BF16) for r, s in zip(rows, shapes)]
        + [dma((chips,))]
        + [dma((k, chips))] * 2
        + [dma((k, 2, 2, chips - 1))] * 2
        + [dma((2,))]
    )

    def kernel(*refs):
        own, made, tiles = refs[7:10]
        last_kernel(n, refs[:4], refs[4:7], own, made, tiles, refs[10:13], refs[13:16], refs[16:])

    hbm, vmem = pl.BlockSpec(memory_space=pl.ANY), pl.BlockSpec(memory_space=pltpu.VMEM)
    return pl.pallas_call(
        kernel,
        out_shape=[jax.ShapeDtypeStruct((r, s[1]), BF16) for r, s in zip(rows, shapes)],
        in_specs=[hbm, vmem, hbm, hbm],
        out_specs=[vmem] * k,
        scratch_shapes=scratch,
        compiler_params=pltpu.CompilerParams(collective_id=collective_id, has_side_effects=True, vmem_limit_bytes=62 << 20),
        name="last_gradients",
    )(down, a_t, by_gate, by_up)


def square_kernel(n, *refs):
    ins, out, slots, send, recv = refs[:-4], refs[-4], refs[-3], refs[-2], refs[-1]
    me = lax.axis_index("dp")
    others = [(me + j) % n for j in range(1, n)]
    entry_barrier(others)
    total = jnp.zeros((8, 512), F32)
    for ref in ins:
        rows, cols = ref.shape

        def add(c, total, ref=ref, cols=cols):
            row = pl.multiple_of(c // (cols // 512) * 16, 16)
            g = ref[pl.ds(row, 16), pl.ds(pl.multiple_of(c % (cols // 512) * 512, 512), 512)].astype(F32)
            return total + g[:8] * g[:8] + g[8:] * g[8:]

        total = lax.fori_loop(0, rows // 16 * (cols // 512), add, total)
    slots[0] = jnp.broadcast_to(jnp.sum(jnp.sum(total, 1, keepdims=True), 0, keepdims=True), (8, 128))
    copies = [remote(slots.at[0], slots.at[j], send.at[j], recv.at[j], d) for j, d in enumerate(others, 1)]
    for c in copies:
        c.start()
    for c in copies:
        c.wait_send()
        c.wait_recv()
    total = slots[0]
    for j in range(1, n):
        total += slots[j]
    out[...] = total


def sum_of_squares(n, blocks, collective_id):
    return pl.pallas_call(
        functools.partial(square_kernel, n),
        out_shape=jax.ShapeDtypeStruct((8, 128), F32),
        in_specs=[pl.BlockSpec(memory_space=pltpu.VMEM)] * len(blocks),
        out_specs=pl.BlockSpec(memory_space=pltpu.VMEM),
        scratch_shapes=[pltpu.VMEM((n, 8, 128), F32)] + [pltpu.SemaphoreType.DMA((n,))] * 2,
        compiler_params=pltpu.CompilerParams(collective_id=collective_id, has_side_effects=True),
        name="sum_of_squares",
    )(*blocks)[0, 0]


def solution(mesh):
    n = mesh.shape["dp"]

    def body(x, dy, wg, wu, wd, *mv):
        h0, dy = x[0], dy[0]
        m, v = mv[:3], mv[3:]

        def scatter_by_xla(g):
            return lax.psum_scatter(g, "dp", scatter_dimension=0, tiled=True)

        a0 = normed(h0)
        g0, u0 = dot(a0, wg[0], 1, 0), dot(a0, wu[0], 1, 0)
        hid0 = act(g0, u0)
        h1 = h0 + dot(hid0, wd[0], 1, 0).astype(BF16)
        a1, norm_back = jax.vjp(normed, h1)
        g1, u1 = dot(a1, wg[1], 1, 0), dot(a1, wu[1], 1, 0)
        hid1 = act(g1, u1)
        grad = lambda a, b: dot(a, b, 0, 0).astype(BF16)
        t_down1 = grad(hid1, dy)
        d_down1 = scatter_by_xla(t_down1)
        dy, _ = lax.optimization_barrier((dy, t_down1))
        dhid1 = dot(dy, wd[1], 1, 1).astype(BF16)
        dg1, du1 = act_back(g1, u1, dhid1)
        t_gate1 = grad(a1, dg1)
        d_gate1 = scatter_by_xla(t_gate1)
        t_up1 = grad(a1, du1)
        d_up1 = scatter_by_xla(t_up1)
        dg1, du1, _, _ = lax.optimization_barrier((dg1, du1, t_gate1, t_up1))
        da1 = dot(dg1, wg[1], 1, 1).astype(BF16) + dot(du1, wu[1], 1, 1).astype(BF16)
        dh1 = dy + norm_back(da1)[0]
        t_down0 = grad(hid0, dh1)
        dhid0 = dot(dh1, wd[0], 1, 1).astype(BF16)
        dg0, du0 = act_back(g0, u0, dhid0)
        d_down0, d_gate0, d_up0 = last_gradients(n, t_down0, a0.T, dg0, du0, 1)
        gs = [(d_gate0, d_gate1), (d_up0, d_up1), (d_down0, d_down1)]
        total = sum_of_squares(n, [g for pair in gs for g in pair], 2)
        count = sum(w.size for w in (wg, wu, wd))
        factor = jnp.minimum(1.0, 0.5 * lax.rsqrt(total / count + 1e-30))
        me = lax.axis_index("dp")
        news, ms, vs = [], [], []
        for w, mm, vv, pair in zip((wg, wu, wd), m, v, gs):
            rows = w.shape[1] // n
            own = lax.dynamic_slice_in_dim(w, me * rows, rows, 1)
            g = jnp.stack([p.astype(F32) for p in pair]) * factor
            new, nm, nv = adamw(own.astype(F32), mm, vv, g)
            news.append(new)
            ms.append(nm)
            vs.append(nv)
        return (*gather(n, news, 0), *ms, *vs)

    seq, whole, shard = P(("rep", "dp")), P(), P(None, "dp")
    return jax.shard_map(
        body,
        mesh=mesh,
        in_specs=(seq, seq, whole, whole, whole, *([shard] * 6)),
        out_specs=(*([P("rep")] * 3), *([P("rep", "dp")] * 6)),
        check_vma=False,
    )
```

```python
import functools

import jax
import jax.numpy as jnp
from jax import lax
from jax.experimental import pallas as pl
from jax.experimental.pallas import tpu as pltpu
from jax.sharding import PartitionSpec as P

F32, BF16 = jnp.float32, jnp.bfloat16
MESH = pl.DeviceIdType.MESH
TILE = 512


def dot(a, b, ca, cb):
    return lax.dot_general(a, b, (((ca,), (cb,)), ((), ())), preferred_element_type=F32)


def normed(h):
    wide = h.astype(F32)
    scale = lax.rsqrt(jnp.mean(wide**2, -1, keepdims=True) + 1e-6)
    return (wide * scale).astype(BF16)


def act(gate, up):
    return (jax.nn.silu(gate) * up).astype(BF16)


def act_back(gate, up, dhid):
    d = dhid.astype(F32)
    s = jax.nn.sigmoid(gate)
    silu = gate * s
    return (d * up * (s * (1 + gate * (1 - s)))).astype(BF16), (d * silu).astype(BF16)


def adamw(w, m, v, g):
    m = 0.9 * m + 0.1 * g
    v = 0.95 * v + 0.05 * g * g
    step = m * lax.rsqrt(v + 1e-8) + 0.1 * w
    return (w - 0.02 * step).astype(BF16), m, v


def place(n):
    me = lax.axis_index("dp")
    core, chip = me % 2, me // 2
    half = n // 4
    pos = chip + (chip // half) * (3 * half - 1 - 2 * chip)

    def owner(p, c):
        return 2 * (p + (p // half) * (3 * half - 1 - 2 * p)) + c

    return core, pos, owner


def entry_barrier(devices):
    sem = pltpu.get_barrier_semaphore()
    for d in devices:
        pl.semaphore_signal(sem, inc=1, device_id={"dp": d}, device_id_type=MESH)
    pl.semaphore_wait(sem, len(devices))


def remote(src, dst, send, recv, dev):
    return pltpu.make_async_remote_copy(
        src_ref=src, dst_ref=dst, send_sem=send, recv_sem=recv, device_id={"dp": dev}, device_id_type=MESH
    )


def gather_kernel(n, rows, *refs):
    k = len(rows)
    ins, outs, bufs = refs[:k], refs[k : 2 * k], refs[2 * k : 3 * k]
    ring_send, ring_recv, d2d_send, d2d_recv, local = refs[3 * k :]
    chips = n // 2
    core, pos, owner = place(n)
    right, left = owner((pos + 1) % chips, core), owner((pos + chips - 1) % chips, core)
    partner = owner(pos, 1 - core)
    entry_barrier((left, right, partner))
    to = (right, left)

    def out_rows(i, way, s, c):
        q = (pos + (chips - s if way == 0 else s)) % chips
        h = rows[i] // 2
        return outs[i].at[:, pl.ds(pl.multiple_of(owner(q, c) * rows[i] + way * h, h), h)]

    def hop(i, way, s):
        return remote(bufs[i].at[way, s], bufs[i].at[way, s + 1], ring_send.at[i, way, s], ring_recv.at[i, way, s], to[way])

    def across(i, way, s, c):
        return remote(bufs[i].at[way, s], out_rows(i, way, s, c), d2d_send.at[i, way, s], d2d_recv.at[i, way, s], partner)

    def keep(i, way, s):
        return pltpu.make_async_copy(bufs[i].at[way, s], out_rows(i, way, s, core), local.at[i, way, s])

    def load(i, way):
        h = rows[i] // 2
        return pltpu.make_async_copy(ins[i].at[:, pl.ds(way * h, h)], bufs[i].at[way, 0], local.at[i, way, chips])

    every = [(i, way) for i in range(k) for way in range(2)]
    for i, way in every:
        load(i, way).start()
    for s in range(chips):
        for i, way in every:
            if s == 0:
                load(i, way).wait()
            else:
                hop(i, way, s - 1).wait_recv()
            if s < chips - 1:
                hop(i, way, s).start()
            across(i, way, s, core).start()
            keep(i, way, s).start()
    for s in range(chips):
        for i, way in every:
            if s < chips - 1:
                hop(i, way, s).wait_send()
            across(i, way, s, core).wait_send()
            across(i, way, s, 1 - core).wait_recv()
            keep(i, way, s).wait()


def gather(n, blocks, collective_id):
    k, chips = len(blocks), n // 2
    rows = [b.shape[1] for b in blocks]
    sems = [pltpu.SemaphoreType.DMA((k, 2, chips))] * 4 + [pltpu.SemaphoreType.DMA((k, 2, chips + 1))]
    return pl.pallas_call(
        functools.partial(gather_kernel, n, rows),
        out_shape=[jax.ShapeDtypeStruct((b.shape[0], n * b.shape[1], b.shape[2]), b.dtype) for b in blocks],
        in_specs=[pl.BlockSpec(memory_space=pl.ANY)] * k,
        out_specs=[pl.BlockSpec(memory_space=pl.ANY)] * k,
        scratch_shapes=[pltpu.VMEM((2, chips, b.shape[0], b.shape[1] // 2, b.shape[2]), b.dtype) for b in blocks] + sems,
        compiler_params=pltpu.CompilerParams(collective_id=collective_id, has_side_effects=True, vmem_limit_bytes=60 << 20),
        name="gather_weights",
    )(*blocks)


def summed(refs, cols, step=512):
    total = refs[0][:, pl.ds(cols, step)].astype(F32)
    for r in refs[1:]:
        total += r[:, pl.ds(cols, step)].astype(F32)
    return total


def last_kernel(n, refs_in, refs_out, total_ref, own, made, tiles, got, buf, slots, sems):
    down, early, a_t, *by_hidden = refs_in[:5]
    done = refs_in[5:]
    own_sem, d2d_send, d2d_recv, ring_send, ring_recv, tile_sem, total_send, total_recv, credit = sems
    chips, k = n // 2, 4
    me = lax.axis_index("dp")
    others = [(me + j) % n for j in range(1, n)]
    grads = (down, made.at[0], made.at[1], early)
    own, got, buf = {0: own[0], 3: own[1]}, (*got, got[2]), (*buf, buf[2])
    rows = [g.shape[0] // n for g in grads]
    wide = [g.shape[1] // 2 for g in grads]
    core, pos, owner = place(n)
    right, left = owner((pos + 1) % chips, core), owner((pos + chips - 1) % chips, core)
    partner = owner(pos, 1 - core)
    entry_barrier(others)
    to = (right, left)

    def start_row(i, d, c, more=0):
        at = owner((pos + d) % chips, c) * rows[i] + more
        return pl.multiple_of(at, rows[i] // 2)

    def load(i, d):
        return pltpu.make_async_copy(grads[i].at[pl.ds(start_row(i, d, core), rows[i])], own[i].at[d], own_sem.at[i, d])

    def cross(i, d):
        src = grads[i].at[pl.ds(start_row(i, d, 1 - core), rows[i])]
        return remote(src, got[i].at[d], d2d_send.at[i, d], d2d_recv.at[i, d], partner)

    def hop(i, part, way, s):
        cols = pl.ds(part * wide[i], wide[i])
        return remote(
            buf[i].at[way, s, :, cols],
            buf[i].at[way, s + 1, :, cols],
            ring_send.at[i, part, way, s],
            ring_recv.at[i, part, way, s],
            to[way],
        )

    order = list(dict.fromkeys(d % chips for s in range(chips) for d in (chips - 1 - s, 1 + s)))

    def begin(i):
        for d in order:
            cross(i, d).start()
            if i in own:
                load(i, d).start()

    ready = set()

    def turn(i, number):
        part, s = number % 2, number // 2
        h = rows[i] // 2
        for way in range(2):
            d = (chips - 1 - s if way == 0 else 1 + s) % chips
            if (i, d) not in ready:
                ready.add((i, d))
                if i in own:
                    load(i, d).wait()
                cross(i, d).wait_recv()
            if s > 0:
                hop(i, part, way, s - 1).wait_recv()
            half = pl.ds(way * h, h)
            mine = own[i].at[d, half] if i in own else grads[i].at[pl.ds(start_row(i, d, core, way * h), h)]
            terms = [mine, got[i].at[d, half]] + ([buf[i].at[way, s]] if s > 0 else [])
            result = buf[i].at[way, s] if s < chips - 1 else refs_out[i].at[half]

            def add(c, _, terms=terms, result=result, part=part, i=i):
                at = pl.multiple_of(part * wide[i] + c * 512, 512)
                result[:, pl.ds(at, 512)] = summed(terms, at).astype(BF16)
                return 0

            lax.fori_loop(0, wide[i] // 512, add, 0)
            if s < chips - 1:
                hop(i, part, way, s).start()

    per = by_hidden[0].shape[1] // TILE
    count = 2 * per

    def fetch(t):
        src = by_hidden[t // per].at[:, pl.ds(t % per * TILE, TILE)]
        return pltpu.make_async_copy(src, tiles.at[t % 2], tile_sem.at[t % 2])

    high = min(512, a_t.shape[0])

    def squares(refs):
        total = jnp.zeros((8, 512), F32)
        for ref in refs:
            across = ref.shape[1] // 512

            def add(c, total, ref=ref, across=across):
                row = pl.multiple_of(c // across * 16, 16)
                g = ref[pl.ds(row, 16), pl.ds(pl.multiple_of(c % across * 512, 512), 512)].astype(F32)
                return total + g[:8] * g[:8] + g[8:] * g[8:]

            total = lax.fori_loop(0, ref.shape[0] // 16 * across, add, total)
        return total

    begin(0)
    begin(3)
    fetch(0).start()
    gate, up = list(range(2 * chips)), list(range(2 * chips))
    for t in range(count):
        fetch(t).wait()
        if t + 1 < count:
            fetch(t + 1).start()

        def matmul(m, _, t=t):
            at = pl.ds(pl.multiple_of(m * high, high), high)
            made[t // per, at, pl.ds(t % per * TILE, TILE)] = jnp.dot(
                a_t[at], tiles[t % 2], preferred_element_type=F32
            ).astype(BF16)
            return 0

        lax.fori_loop(0, a_t.shape[0] // high, matmul, 0)
        for number in range(t * 2 * chips // count, (t + 1) * 2 * chips // count):
            turn(0, number)
            turn(3, number)
        if t == per - 1:
            begin(1)
    for part in range(2):
        for way in range(2):
            for s in range(chips - 1):
                hop(3, part, way, s).wait_send()
    for d in (left, right, partner):
        pl.semaphore_signal(credit, inc=1, device_id={"dp": d}, device_id_type=MESH)
    turn(1, gate.pop(0))
    turn(1, gate.pop(0))
    pl.semaphore_wait(credit, 3)
    begin(2)
    turn(1, gate.pop(0))
    turn(1, gate.pop(0))
    total = squares([refs_out[0], refs_out[3], *done])
    while gate or up:
        if gate:
            turn(1, gate.pop(0))
        if up:
            turn(2, up.pop(0))
    total += squares(refs_out[1:3])
    slots[0] = jnp.broadcast_to(jnp.sum(jnp.sum(total, 1, keepdims=True), 0, keepdims=True), (8, 128))
    copies = [remote(slots.at[0], slots.at[j], total_send.at[j], total_recv.at[j], d) for j, d in enumerate(others, 1)]
    for c in copies:
        c.start()
    for i in range(k):
        for d in range(chips):
            cross(i, d).wait_send()
        for part in range(2) if i < 3 else ():
            for way in range(2):
                for s in range(chips - 1):
                    hop(i, part, way, s).wait_send()
    for c in copies:
        c.wait_send()
        c.wait_recv()
    total = slots[0]
    for j in range(1, n):
        total += slots[j]
    total_ref[...] = total


def last_gradients(n, down, early, a_t, by_gate, by_up, done, collective_id):
    chips, k = n // 2, 4
    shapes = [down.shape, (a_t.shape[0], by_gate.shape[1]), (a_t.shape[0], by_up.shape[1]), early.shape]
    rows = [s[0] // n for s in shapes]
    dma = pltpu.SemaphoreType.DMA
    scratch = (
        [pltpu.VMEM((chips, rows[i], shapes[i][1]), BF16) for i in (0, 3)]
        + [pltpu.VMEM((2, *shapes[1]), BF16), pltpu.VMEM((2, a_t.shape[1], TILE), BF16)]
        + [pltpu.VMEM((chips, r, s[1]), BF16) for r, s in zip(rows[:3], shapes)]
        + [pltpu.VMEM((2, chips, r // 2, s[1]), BF16) for r, s in zip(rows[:3], shapes)]
        + [pltpu.VMEM((n, 8, 128), F32)]
        + [dma((k, chips))]
        + [dma((k, chips))] * 2
        + [dma((k, 2, 2, chips - 1))] * 2
        + [dma((2,))]
        + [dma((n,))] * 2
        + [pltpu.SemaphoreType.REGULAR]
    )
    count = 5 + len(done)

    def kernel(*refs):
        ins, outs, total, refs = refs[:count], refs[count : count + k], refs[count + k], refs[count + k + 1 :]
        last_kernel(n, ins, outs, total, refs[:2], refs[2], refs[3], refs[4:7], refs[7:10], refs[10], refs[11:])

    hbm, vmem = pl.BlockSpec(memory_space=pl.ANY), pl.BlockSpec(memory_space=pltpu.VMEM)
    return pl.pallas_call(
        kernel,
        out_shape=[jax.ShapeDtypeStruct((r, s[1]), BF16) for r, s in zip(rows, shapes)] + [jax.ShapeDtypeStruct((8, 128), F32)],
        in_specs=[hbm, hbm, vmem, hbm, hbm] + [vmem] * len(done),
        out_specs=[vmem] * (k + 1),
        scratch_shapes=scratch,
        compiler_params=pltpu.CompilerParams(collective_id=collective_id, has_side_effects=True, vmem_limit_bytes=62 << 20),
        name="last_gradients",
    )(down, early, a_t, by_gate, by_up, *done)


def solution(mesh):
    n = mesh.shape["dp"]

    def body(x, dy, wg, wu, wd, *mv):
        h0, dy = x[0], dy[0]
        m, v = mv[:3], mv[3:]

        def scatter_by_xla(g):
            return lax.psum_scatter(g, "dp", scatter_dimension=0, tiled=True)

        a0 = normed(h0)
        g0, u0 = dot(a0, wg[0], 1, 0), dot(a0, wu[0], 1, 0)
        hid0 = act(g0, u0)
        h1 = h0 + dot(hid0, wd[0], 1, 0).astype(BF16)
        a1, norm_back = jax.vjp(normed, h1)
        g1, u1 = dot(a1, wg[1], 1, 0), dot(a1, wu[1], 1, 0)
        hid1 = act(g1, u1)
        grad = lambda a, b: dot(a, b, 0, 0).astype(BF16)
        t_down1 = grad(hid1, dy)
        d_down1 = scatter_by_xla(t_down1)
        dy, _ = lax.optimization_barrier((dy, t_down1))
        dhid1 = dot(dy, wd[1], 1, 1).astype(BF16)
        dg1, du1 = act_back(g1, u1, dhid1)
        t_gate1 = grad(a1, dg1)
        d_gate1 = scatter_by_xla(t_gate1)
        t_up1 = grad(a1, du1)
        dg1, du1, _, _ = lax.optimization_barrier((dg1, du1, t_gate1, t_up1))
        da1 = dot(dg1, wg[1], 1, 1).astype(BF16) + dot(du1, wu[1], 1, 1).astype(BF16)
        dh1 = dy + norm_back(da1)[0]
        t_down0 = grad(hid0, dh1)
        dhid0 = dot(dh1, wd[0], 1, 1).astype(BF16)
        dg0, du0 = act_back(g0, u0, dhid0)
        d_down0, d_gate0, d_up0, d_up1, total = last_gradients(n, t_down0, t_up1, a0.T, dg0, du0, (d_down1, d_gate1), 1)
        gs = [(d_gate0, d_gate1), (d_up0, d_up1), (d_down0, d_down1)]
        total = total[0, 0]
        count = sum(w.size for w in (wg, wu, wd))
        factor = jnp.minimum(1.0, 0.5 * lax.rsqrt(total / count + 1e-30))
        me = lax.axis_index("dp")
        news, ms, vs = [], [], []
        for w, mm, vv, pair in zip((wg, wu, wd), m, v, gs):
            rows = w.shape[1] // n
            own = lax.dynamic_slice_in_dim(w, me * rows, rows, 1)
            g = jnp.stack([p.astype(F32) for p in pair]) * factor
            new, nm, nv = adamw(own.astype(F32), mm, vv, g)
            news.append(new)
            ms.append(nm)
            vs.append(nv)
        return (*gather(n, news, 0), *ms, *vs)

    seq, whole, shard = P(("rep", "dp")), P(), P(None, "dp")
    return jax.shard_map(
        body,
        mesh=mesh,
        in_specs=(seq, seq, whole, whole, whole, *([shard] * 6)),
        out_specs=(*([P("rep")] * 3), *([P("rep", "dp")] * 6)),
        check_vma=False,
    )
```
